32 devices in a mesh: fsdp: 2 (over y), ctx: 4 (over z), tp: 4 (over x, core).
Axes of the slice: x: 2, y: 2, z: 4, core: 2. Of those that a mesh axis runs over, the one named last changes fastest.
Arguments:
- layer_input: bfloat16 [8, 2048, 768], P('fsdp', ('ctx', 'tp')), may hold values from -6 to 6
- cotangent: bfloat16 [8, 2048, 768], P('fsdp', 'ctx'), may hold values from -6 to 6
- picture_ids: int32 [8, 2048], P('fsdp', 'ctx'), may hold values from -1 to 19, as said below
- ln1_gain: float32 [768], replicated, may hold values from 0.25 to 1.75
- ln1_bias: float32 [768], replicated, may hold values from -3 to 3
- w_query: bfloat16 [768, 768], P('fsdp', 'tp'), may hold values from -0.21875 to 0.21875
- w_key: bfloat16 [768, 768], P('fsdp', 'tp'), may hold values from -0.21875 to 0.21875
- w_value: bfloat16 [768, 768], P('fsdp', 'tp'), may hold values from -0.21875 to 0.21875
- query_gain: float32 [64], replicated, may hold values from 0.25 to 1.75
- key_gain: float32 [64], replicated, may hold values from 0.25 to 1.75
- w_out: bfloat16 [768, 768], P('tp', 'fsdp'), may hold values from -1.25 to 1.25
- ln2_gain: float32 [768], replicated, may hold values from 0.25 to 1.75
- ln2_bias: float32 [768], replicated, may hold values from -3 to 3
- w_hidden: bfloat16 [768, 3072], P('fsdp', 'tp'), may hold values from -0.21875 to 0.21875
- hidden_bias: float32 [3072], P('tp'), may hold values from -3 to 3
- w_back: bfloat16 [3072, 768], P('tp', 'fsdp'), may hold values from -0.109375 to 0.109375
- out_bias: float32 [768], replicated, may hold values from -3 to 3
Outputs:
- layer_output: bfloat16 [8, 2048, 768], P('fsdp', ('ctx', 'tp'))
- input_grad: bfloat16 [8, 2048, 768], P('fsdp', ('ctx', 'tp'))
- ln1_gain_grad: float32 [768], replicated
- ln1_bias_grad: float32 [768], replicated
- w_query_grad: float32 [768, 768], P(('fsdp', 'ctx'), 'tp')
- w_key_grad: float32 [768, 768], P(('fsdp', 'ctx'), 'tp')
- w_value_grad: float32 [768, 768], P(('fsdp', 'ctx'), 'tp')
- query_gain_grad: float32 [64], replicated
- key_gain_grad: float32 [64], replicated
- w_out_grad: float32 [768, 768], P('tp', ('fsdp', 'ctx'))
- ln2_gain_grad: float32 [768], replicated
- ln2_bias_grad: float32 [768], replicated
- w_hidden_grad: float32 [768, 3072], P(('fsdp', 'ctx'), 'tp')
- hidden_bias_grad: float32 [3072], P('tp')
- w_back_grad: float32 [3072, 768], P('tp', ('fsdp', 'ctx'))
- out_bias_grad: float32 [768], replicated
The draws below stay inside these ranges and needn't reach their ends.
Inputs may be any that keep to these rules, and one draw needn't show every extreme that they name: `picture_ids`: each row holds pictures of 100 to 1024 consecutive positions numbered 0, 1, 2, ... from the row's start, then padding of -1 to the row's end; every row ends with at least one padding position; the first row holds only pictures of 100 positions, as many as fit before its last position.
All inputs are finite; a program needn't handle non-finite values.
Results may differ from the reference program's by a relative error of at most 0.028.
Values may be sent and summed in bfloat16 or wider, within the bound.
A program may use at most 128 MiB of HBM per device.

```python
import jax
import jax.numpy as jnp
from jax import lax

D = 768
H = 12
HD = 64
FF = 3072
ROW = 2048
PIC_MIN = 100
PIC_MAX = 1024
ROWS = 8
MAXPICS = 21


def draw_picture_ids(key, part):
    random_lens = jax.random.randint(key, (ROWS, MAXPICS), PIC_MIN, PIC_MAX + 1).astype(jnp.int32)
    row_numbers = jnp.arange(ROWS, dtype=jnp.int32)
    picture_lens = jnp.where(row_numbers[:, None] == 0, jnp.int32(PIC_MIN), random_lens).astype(jnp.int32)
    picture_ends = jnp.cumsum(picture_lens, axis=1).astype(jnp.int32)
    places = jnp.arange(ROW, dtype=jnp.int32)
    fitting = picture_ends <= ROW - 1
    row_limit = jnp.max(jnp.where(fitting, picture_ends, 0), axis=1)
    passed = (places[None, :, None] >= picture_ends[:, None, :]).astype(jnp.int32)
    numbers = jnp.sum(passed, axis=2).astype(jnp.int32)
    return jnp.where(places[None, :] < row_limit[:, None], numbers, -1).astype(jnp.int32)


def shard_levels(key, dims, split, smallest, top_value):
    def one(position, parts):
        heights = jax.random.uniform(jax.random.fold_in(jax.random.fold_in(key, 6), position), (parts,), jnp.float32, smallest / len(split), top_value / len(split))
        return jnp.repeat(jnp.exp(heights), dims[position] // parts).reshape((-1,) + (1,) * (len(dims) - position - 1))

    loudness = one(*split[0])
    for cut in split[1:]:
        loudness = loudness * one(*cut)
    return loudness


def bell_draw(own_key, shape, width, reach, shards=(), kind=jnp.bfloat16):
    level = shard_levels(own_key, shape, shards, -0.22, 0.18) if shards else 1.0
    array = jax.random.normal(own_key, shape, jnp.float32) * width * level
    return jnp.minimum(jnp.maximum(array, -reach), reach).astype(kind)


def setup_inputs(seed: int = 0) -> dict:
    key_list = jax.random.split(jax.random.key(seed), 18)
    return {
        "layer_input": bell_draw(key_list[0], (ROWS, ROW, D), 1.0, 6.0, ((0, 2), (1, 16))),
        "cotangent": bell_draw(key_list[1], (ROWS, ROW, D), 1.0, 6.0, ((0, 2), (1, 4))),
        "picture_ids": draw_picture_ids(jax.random.fold_in(key_list[17], 71), 0),
        "ln1_gain": jnp.clip(1.0 + 0.15 * jax.random.normal(key_list[3], (D,), jnp.float32), 0.25, 1.75),
        "ln1_bias": bell_draw(key_list[4], (D,), 0.3, 3.0, (), jnp.float32),
        "w_query": bell_draw(key_list[5], (D, D), D ** -0.5, 0.21875, ((0, 2), (1, 4))),
        "w_key": bell_draw(key_list[6], (D, D), D ** -0.5, 0.21875, ((0, 2), (1, 4))),
        "w_value": bell_draw(key_list[7], (D, D), D ** -0.5, 0.21875, ((0, 2), (1, 4))),
        "query_gain": jnp.clip(1.0 + 0.15 * jax.random.normal(key_list[8], (HD,), jnp.float32), 0.25, 1.75),
        "key_gain": jnp.clip(1.0 + 0.15 * jax.random.normal(key_list[9], (HD,), jnp.float32), 0.25, 1.75),
        "w_out": bell_draw(key_list[10], (D, D), (D // 32) ** -0.5, 1.25, ((0, 4), (1, 2))),
        "ln2_gain": jnp.clip(1.0 + 0.15 * jax.random.normal(key_list[11], (D,), jnp.float32), 0.25, 1.75),
        "ln2_bias": bell_draw(key_list[12], (D,), 0.3, 3.0, (), jnp.float32),
        "w_hidden": bell_draw(key_list[13], (D, FF), D ** -0.5, 0.21875, ((0, 2), (1, 4))),
        "hidden_bias": bell_draw(key_list[14], (FF,), 0.3, 3.0, ((0, 4),), jnp.float32),
        "w_back": bell_draw(key_list[15], (FF, D), FF ** -0.5, 0.109375, ((0, 4), (1, 2))),
        "out_bias": bell_draw(key_list[16], (D,), 0.3, 3.0, (), jnp.float32),
    }


@jax.custom_vjp
def low(v):
    return lax.optimization_barrier(v.astype(jnp.bfloat16)).astype(jnp.float32)

@jax.custom_vjp
def low_back(v):
    return v

def low_keep(v):
    return (low(v), None)

def low_pass(kept, grad):
    return (grad,)

def back_keep(v):
    return (v, None)

def back_low(kept, grad):
    return (low(grad),)
low.defvjp(low_keep, low_pass)
low_back.defvjp(back_keep, back_low)
MASKED = -1e+30
EPSILON = 1e-06

def layer_norm(values, gain_vec, bias_vec):
    row_mean = lax.optimization_barrier(jnp.mean(values, axis=-1, keepdims=True))
    centred = values - row_mean
    variance = lax.optimization_barrier(jnp.mean(centred * centred, axis=-1, keepdims=True))
    return centred * lax.rsqrt(variance + EPSILON) * gain_vec + bias_vec

def head_norm(values, gain_vec):
    row_mean = lax.optimization_barrier(jnp.mean(values, axis=-1, keepdims=True))
    centred = values - row_mean
    variance = lax.optimization_barrier(jnp.mean(centred * centred, axis=-1, keepdims=True))
    return centred * lax.rsqrt(variance + EPSILON) * gain_vec

def matmul(left, right):
    return jnp.dot(left, right, precision=lax.Precision.HIGHEST)

def attend_block(query_block, ids_query, keys_all, values_all, ids_keys):
    scores = jnp.einsum('hqd,hkd->hqk', query_block, keys_all, precision=lax.Precision.HIGHEST) * HD ** (-0.5)
    scores = low_back(scores)
    allowed = (ids_query[:, None] == ids_keys[None, :]) & (ids_query[:, None] >= 0)
    row_top = lax.optimization_barrier(jnp.max(jnp.where(allowed, scores, MASKED), axis=-1, keepdims=True))
    expo_vals = jnp.exp(jnp.where(allowed, scores - row_top, MASKED))
    row_total = jnp.maximum(lax.optimization_barrier(jnp.sum(expo_vals, axis=-1, keepdims=True)), 1.0)
    weights = low(expo_vals / row_total)
    return jnp.einsum('hqk,hkd->qhd', weights, values_all, precision=lax.Precision.HIGHEST)
checked_block = jax.checkpoint(attend_block)

def row_forward(row_in, ids_row, params):
    gain_one, bias_one, w_q, w_k, w_v, gain_q, gain_k, w_o, gain_two, bias_two, w_h, bias_h, w_b, bias_b = params
    normed = low(layer_norm(row_in, gain_one, bias_one))
    raw_q = low_back(matmul(normed, w_q))
    raw_k = low_back(matmul(normed, w_k))
    raw_v = low_back(matmul(normed, w_v))
    query_heads = low(head_norm(raw_q.reshape(ROW, H, HD), gain_q)).transpose(1, 0, 2)
    key_heads = low(head_norm(raw_k.reshape(ROW, H, HD), gain_k)).transpose(1, 0, 2)
    value_heads = low(raw_v.reshape(ROW, H, HD)).transpose(1, 0, 2)
    block_len = min(512, ROW)
    query_blocks = query_heads.reshape(H, ROW // block_len, block_len, HD).transpose(1, 0, 2, 3)
    id_blocks = ids_row.reshape(ROW // block_len, block_len)
    attended = lax.map(lambda bundle: checked_block(bundle[0], bundle[1], key_heads, value_heads, ids_row), (query_blocks, id_blocks))
    attended = low(low_back(attended.reshape(ROW, D)))
    attn_out = low_back(matmul(attended, w_o))
    hidden_in = row_in + attn_out
    mid_normed = low(layer_norm(hidden_in, gain_two, bias_two))
    pre_act = low_back(matmul(mid_normed, w_h) + bias_h)
    activ = low(jax.nn.gelu(pre_act, approximate=False))
    return hidden_in + matmul(activ, w_b) + bias_b

def reference(layer_input, cotangent, picture_ids, ln1_gain, ln1_bias, w_query, w_key, w_value, query_gain, key_gain, w_out, ln2_gain, ln2_bias, w_hidden, hidden_bias, w_back, out_bias):
    params = tuple((item.astype(jnp.float32) for item in (ln1_gain, ln1_bias, w_query, w_key, w_value, query_gain, key_gain, w_out, ln2_gain, ln2_bias, w_hidden, hidden_bias, w_back, out_bias)))

    def row_step(grads, bundle):
        row_in, row_grad, ids_row = bundle

        def forward_fn(value_in, *param_list):
            return row_forward(value_in, ids_row, param_list)
        row_out, pull = jax.vjp(forward_fn, row_in.astype(jnp.float32), *params)
        pulled = pull(row_grad.astype(jnp.float32))
        summed = tuple((old + new for old, new in zip(grads, pulled[1:])))
        return (summed, (row_out.astype(jnp.bfloat16), pulled[0].astype(jnp.bfloat16)))
    zero_grads = tuple((jnp.zeros_like(item) for item in params))
    grads, (outputs, input_grads) = lax.scan(row_step, zero_grads, (layer_input, cotangent, picture_ids))
    return (outputs, input_grads) + grads
```

```python
import functools

import jax
import jax.numpy as jnp
from jax import lax
from jax.experimental import pallas as pl
from jax.experimental.pallas import tpu as pltpu
from jax.sharding import PartitionSpec as P

HD = 64
LANES = 128
EPSILON = 1e-06
FAR = 192.0
F32 = jnp.float32
BF16 = jnp.bfloat16
CELL = 128


def params(grid_len=1):
    return pltpu.CompilerParams(
        dimension_semantics=("arbitrary",) * grid_len, vmem_limit_bytes=56 * 1024 * 1024
    )


def dot(left, right, contract):
    return lax.dot_general(left, right, (contract, ((), ())), preferred_element_type=F32)


NN = ((1,), (0,))
NT = ((1,), (1,))
TN = ((0,), (0,))


def lane_index(rows):
    return lax.broadcasted_iota(jnp.int32, (rows, LANES), 1)


def norm_stats(values, width):
    mean = jnp.sum(values, axis=-1, keepdims=True) * (1.0 / width)
    return mean


def full_norm(values):
    mean = jnp.mean(values, axis=-1, keepdims=True)
    centred = values - mean
    scale = lax.rsqrt(jnp.mean(centred * centred, axis=-1, keepdims=True) + EPSILON)
    return centred * scale, scale


def head_norm(raw, lane):
    mean = jnp.sum(raw, axis=-1, keepdims=True) * (1.0 / HD)
    centred = jnp.where(lane < HD, raw - mean, 0.0)
    scale = lax.rsqrt(jnp.sum(centred * centred, axis=-1, keepdims=True) * (1.0 / HD) + EPSILON)
    return centred * scale, scale


def project_kernel(heads, x_ref, w_ref, g_ref, b_ref, qg_ref, kg_ref, id_ref,
                   n_ref, q_ref, k_ref, v_ref):
    rows = x_ref.shape[0]
    normal, _ = full_norm(x_ref[...].astype(F32))
    normed = (normal * g_ref[...] + b_ref[...]).astype(BF16)
    n_ref[...] = normed
    raw = dot(normed, w_ref[...], NN)
    lane = lane_index(rows)
    ids = id_ref[...]
    hot = (lane == ids + HD) & (ids >= 0)
    tail_q = jnp.where(hot, FAR, jnp.where(lane == LANES - 1, -FAR, 0.0))
    tail_k = jnp.where(hot | (lane == LANES - 1), 1.0, 0.0)
    tail_v = jnp.where((lane == HD) | (lane == HD + 1), 1.0, 0.0)
    for h in range(heads):
        def part(which):
            at = (which * heads + h) * LANES
            return raw[:, at:at + LANES]
        query = head_norm(part(0), lane)[0] * qg_ref[...]
        key = head_norm(part(1), lane)[0] * kg_ref[...]
        query = query.astype(BF16).astype(F32) * HD ** (-0.5)
        q_ref[h] = (query + tail_q).astype(BF16)
        k_ref[h] = (key + tail_k).astype(BF16)
        v_ref[h] = (part(2) + tail_v).astype(BF16)


def project(x, w, gain, bias, qg, kg, ids, heads):
    rows, width = x.shape
    block = 256
    full = lambda shape: pl.BlockSpec(shape, lambda i: (0,) * len(shape))
    heads_spec = pl.BlockSpec((heads, block, LANES), lambda i: (0, i, 0))
    heads_out = jax.ShapeDtypeStruct((heads, rows, LANES), BF16)
    return pl.pallas_call(
        functools.partial(project_kernel, heads),
        grid=(rows // block,),
        in_specs=[pl.BlockSpec((block, width), lambda i: (i, 0)), full(w.shape),
                  full(gain.shape), full(bias.shape), full(qg.shape), full(kg.shape),
                  pl.BlockSpec((block, 1), lambda i: (i, 0))],
        out_specs=[pl.BlockSpec((block, width), lambda i: (i, 0))] + [heads_spec] * 3,
        out_shape=[jax.ShapeDtypeStruct((rows, width), BF16)] + [heads_out] * 3,
        compiler_params=params(),
        cost_estimate=pl.CostEstimate(flops=2 * rows * width * w.shape[1],
                                      bytes_accessed=4 * rows * width, transcendentals=0),
        name="project",
    )(x, w, gain, bias, qg, kg, ids)


def block_of(refs, h, pair, cell):
    at = pl.ds(pl.multiple_of(cell * CELL, CELL), CELL)
    return jnp.concatenate([refs[2 * pair][h, at], refs[2 * pair + 1][h, at]], axis=0)


def attend_kernel(heads, cells, pair, act_ref, *refs):
    q, k, v = refs[0:2], refs[2:6], refs[6:10]
    ob, of, acc = refs[10:12], refs[12:14], refs[14]
    i = pl.program_id(0)
    acc[...] = jnp.zeros_like(acc)
    queries = [jnp.concatenate([q[0][h], q[1][h]], axis=0) for h in range(heads)]
    for kp in range(2):
        def step(c, carry):
            @pl.when(act_ref[pair * cells + i, kp * cells + c] > 0)
            def _():
                for h in range(heads):
                    s = dot(queries[h], block_of(k, h, kp, c), NT)
                    e = jnp.exp(s).astype(BF16)
                    acc[h] += dot(e, block_of(v, h, kp, c), NN)
            return carry
        lax.fori_loop(0, cells, step, 0)
    lane = lane_index(2 * CELL)
    flat = []
    for h in range(heads):
        total = acc[h][:, HD:HD + 1]
        inverse = jnp.where(total > 0.0, 1.0 / jnp.where(total > 0.0, total, 1.0), 0.0)
        out = acc[h] * inverse
        out = jnp.where(lane < HD, out, jnp.where(lane == HD, inverse, 0.0))
        of[0][h] = out[:CELL]
        of[1][h] = out[CELL:]
        flat.append(out[:, :HD])
    flat = jnp.concatenate(flat, axis=1).astype(BF16)
    ob[0][...] = flat[:CELL]
    ob[1][...] = flat[CELL:]


def attend(act, q, k, v, pair, heads, cells):
    rows = cells * CELL
    mine = pl.BlockSpec((heads, CELL, LANES), lambda i, a: (0, i, 0))
    whole = pl.BlockSpec((heads, rows, LANES), lambda i, a: (0, 0, 0))
    return pl.pallas_call(
        functools.partial(attend_kernel, heads, cells, pair),
        grid_spec=pltpu.PrefetchScalarGridSpec(
            num_scalar_prefetch=1, grid=(cells,),
            in_specs=[mine] * 2 + [whole] * 8,
            out_specs=[pl.BlockSpec((CELL, heads * HD), lambda i, a: (i, 0))] * 2 + [mine] * 2,
            scratch_shapes=[pltpu.VMEM((heads, 2 * CELL, LANES), F32)]),
        out_shape=[jax.ShapeDtypeStruct((rows, heads * HD), BF16)] * 2
        + [jax.ShapeDtypeStruct((heads, rows, LANES), F32)] * 2,
        compiler_params=params(),
        cost_estimate=pl.CostEstimate(flops=4 * heads * 8 * rows * rows * 128,
                                      bytes_accessed=heads * rows * 128 * 24, transcendentals=0),
        name="attend%d" % pair,
    )(act, *q[2 * pair:2 * pair + 2], *k, *v)


def attend_back_kernel(heads, cells, act_ref, *refs):
    q, k, v, do, of = refs[0:4], refs[4:8], refs[8:12], refs[12:16], refs[16:20]
    dq, dk, dv = refs[20:24], refs[24:28], refs[28:32]
    acc = refs[32]
    i = pl.program_id(0)
    lane = lane_index(2 * CELL)

    @pl.when(i == 0)
    def _():
        for ref in (*dk, *dv):
            ref[...] = jnp.zeros_like(ref)

    for pair in range(2):
        acc[...] = jnp.zeros_like(acc)
        queries, grads = [], []
        grad_all = jnp.concatenate([do[2 * pair][...], do[2 * pair + 1][...]], axis=0)
        for h in range(heads):
            queries.append(jnp.concatenate([q[2 * pair][h], q[2 * pair + 1][h]], axis=0))
            out = jnp.concatenate([of[2 * pair][h], of[2 * pair + 1][h]], axis=0)
            grad = grad_all[:, h * HD:(h + 1) * HD].astype(F32)
            grad = jnp.concatenate([grad, jnp.zeros_like(grad)], axis=1)
            inverse = out[:, HD:HD + 1]
            grad = grad * inverse
            minus = -jnp.sum(grad * out, axis=-1, keepdims=True)
            high = minus.astype(BF16).astype(F32)
            grad = jnp.where(lane == HD, high, jnp.where(lane == HD + 1, minus - high, grad))
            grads.append(grad.astype(BF16))
        for kp in range(2):
            def step(c, carry):
                @pl.when(act_ref[pair * cells + i, kp * cells + c] > 0)
                def _():
                    at = pl.ds(pl.multiple_of(c * CELL, CELL), CELL)
                    for h in range(heads):
                        keys = block_of(k, h, kp, c)
                        e = jnp.exp(dot(keys, queries[h], NT))
                        dp = dot(block_of(v, h, kp, c), grads[h], NT)
                        ds = (e * dp).astype(BF16)
                        part_v = dot(e.astype(BF16), grads[h], NN)
                        part_k = dot(ds, queries[h], NN)
                        acc[h] += dot(ds, keys, TN)
                        dv[2 * kp][h, at] += part_v[:CELL]
                        dv[2 * kp + 1][h, at] += part_v[CELL:]
                        dk[2 * kp][h, at] += part_k[:CELL]
                        dk[2 * kp + 1][h, at] += part_k[CELL:]
                return carry
            lax.fori_loop(0, cells, step, 0)
        for h in range(heads):
            out = acc[h] * HD ** (-0.5)
            dq[2 * pair][h] = out[:CELL]
            dq[2 * pair + 1][h] = out[CELL:]


def attend_back(act, q, k, v, do, of, heads, cells):
    rows = cells * CELL
    mine = pl.BlockSpec((heads, CELL, LANES), lambda i, a: (0, i, 0))
    whole = pl.BlockSpec((heads, rows, LANES), lambda i, a: (0, 0, 0))
    flat = pl.BlockSpec((CELL, heads * HD), lambda i, a: (i, 0))
    wide = jax.ShapeDtypeStruct((heads, rows, LANES), F32)
    out = pl.pallas_call(
        functools.partial(attend_back_kernel, heads, cells),
        grid_spec=pltpu.PrefetchScalarGridSpec(
            num_scalar_prefetch=1, grid=(cells,),
            in_specs=[mine] * 4 + [whole] * 8 + [flat] * 4 + [mine] * 4,
            out_specs=[mine] * 4 + [whole] * 8,
            scratch_shapes=[pltpu.VMEM((heads, 2 * CELL, LANES), F32)]),
        out_shape=[wide] * 12,
        compiler_params=params(),
        cost_estimate=pl.CostEstimate(flops=10 * heads * 16 * rows * rows * 128,
                                      bytes_accessed=heads * rows * 128 * 80, transcendentals=0),
        name="attend_back",
    )(act, *q, *k, *v, *do, *of)
    return out[0:4], out[4:8], out[8:12]


def feed_kernel(m_ref, dy_ref, wh_ref, wb_ref, hb_ref, act_ref, du_ref, y_ref, dm_ref, gb_ref):
    u = dot(m_ref[...], wh_ref[...], NN) + hb_ref[...]
    half = 0.5 * (1.0 + lax.erf(u * 0.7071067811865476))
    act = (u * half).astype(BF16)
    act_ref[...] = act
    y_ref[...] = dot(act, wb_ref[...], NN).astype(BF16)
    dact = dot(dy_ref[...], wb_ref[...], NT)
    slope = half + u * (jnp.exp(-0.5 * u * u) * 0.3989422804014327)
    du = (dact * slope).astype(BF16)
    du_ref[...] = du
    dm_ref[...] = dot(du, wh_ref[...], NT).astype(BF16)

    @pl.when(pl.program_id(0) == 0)
    def _():
        gb_ref[...] = jnp.zeros_like(gb_ref)
    gb_ref[...] += jnp.sum(du.astype(F32).reshape(-1, 8, du.shape[1]), axis=0)


def feed(mid, dy, wh, wb, hb):
    rows, width = mid.shape
    units = wh.shape[1]
    block = 256
    row = lambda w: pl.BlockSpec((block, w), lambda i: (i, 0))
    full = lambda shape: pl.BlockSpec(shape, lambda i: (0,) * len(shape))
    shape = lambda w: jax.ShapeDtypeStruct((rows, w), BF16)
    return pl.pallas_call(
        feed_kernel, grid=(rows // block,),
        in_specs=[row(width), row(width), full(wh.shape), full(wb.shape), full(hb.shape)],
        out_specs=[row(units), row(units), row(width), row(width), full((8, units))],
        out_shape=[shape(units), shape(units), shape(width), shape(width),
                   jax.ShapeDtypeStruct((8, units), F32)],
        compiler_params=params(),
        cost_estimate=pl.CostEstimate(flops=12 * rows * width * units,
                                      bytes_accessed=12 * rows * width, transcendentals=0),
        name="feed",
    )(mid, dy, wh, wb, hb)


def project_back_kernel(heads, n_ref, w_ref, qg_ref, kg_ref, dq_ref, dk_ref, dv_ref,
                        d_ref, dn_ref, gq_ref, gk_ref):
    rows = n_ref.shape[0]
    lane = lane_index(rows)
    raw = dot(n_ref[...], w_ref[:, :2 * heads * LANES], NN)

    @pl.when(pl.program_id(0) == 0)
    def _():
        gq_ref[...] = jnp.zeros_like(gq_ref)
        gk_ref[...] = jnp.zeros_like(gk_ref)

    wide, thin = [], []
    for which, (g_ref, d_in, acc) in enumerate(
            ((qg_ref, dq_ref, gq_ref), (kg_ref, dk_ref, gk_ref))):
        for h in range(heads):
            at = (which * heads + h) * LANES
            normal, scale = head_norm(raw[:, at:at + LANES], lane)
            grad = jnp.where(lane < HD, d_in[h], 0.0)
            acc[...] += jnp.sum((grad * normal).reshape(-1, 8, LANES), axis=0)
            f = grad * g_ref[...]
            mean_f = jnp.sum(f, axis=-1, keepdims=True) * (1.0 / HD)
            mean_fn = jnp.sum(f * normal, axis=-1, keepdims=True) * (1.0 / HD)
            out = jnp.where(lane < HD, scale * (f - mean_f - normal * mean_fn), 0.0)
            wide.append(out.astype(BF16))
    for h in range(heads):
        wide.append(jnp.where(lane < HD, dv_ref[h], 0.0).astype(BF16))
    dn_ref[...] = dot(jnp.concatenate(wide, axis=1), w_ref[...], NT).astype(BF16)
    d_ref[...] = jnp.concatenate([item[:, :HD] for item in wide], axis=1)


def project_back(normed, w, qg, kg, dq, dk, dv, heads):
    rows, width = normed.shape
    block = 256
    row = lambda wd: pl.BlockSpec((block, wd), lambda i: (i, 0))
    full = lambda shape: pl.BlockSpec(shape, lambda i: (0,) * len(shape))
    hs = pl.BlockSpec((heads, block, LANES), lambda i: (0, i, 0))
    return pl.pallas_call(
        functools.partial(project_back_kernel, heads), grid=(rows // block,),
        in_specs=[row(width), full(w.shape), full(qg.shape), full(kg.shape), hs, hs, hs],
        out_specs=[row(3 * heads * HD), row(width), full((8, LANES)), full((8, LANES))],
        out_shape=[jax.ShapeDtypeStruct((rows, 3 * heads * HD), BF16),
                   jax.ShapeDtypeStruct((rows, width), BF16),
                   jax.ShapeDtypeStruct((8, LANES), F32), jax.ShapeDtypeStruct((8, LANES), F32)],
        compiler_params=params(),
        cost_estimate=pl.CostEstimate(flops=4 * rows * width * w.shape[1],
                                      bytes_accessed=6 * rows * width, transcendentals=0),
        name="project_back",
    )(normed, w, qg, kg, dq, dk, dv)


def solution(mesh):
    fsdp, ctx, tp = mesh.shape["fsdp"], mesh.shape["ctx"], mesh.shape["tp"]

    def hop(value, axis, bit):
        size = mesh.shape[axis]
        return lax.ppermute(value, axis, [(i, i ^ bit) for i in range(size)])

    def shift(value, by):
        return lax.ppermute(value, "ctx", [(i, (i + by) % ctx) for i in range(ctx)])

    def pick(value, index):
        return lax.dynamic_index_in_dim(value, index, 0, keepdims=False)

    def gather_tp(own):
        near = hop(own, "tp", 1)
        far = hop(own, "tp", 2)
        return [own, near, far, hop(far, "tp", 1)]

    def add_low(left, right):
        return (left.astype(F32) + right.astype(F32)).astype(BF16)

    def scatter_tp(pieces):
        third = hop(pieces[3], "tp", 1)
        second = add_low(pieces[2], third)
        far = hop(second, "tp", 2)
        near = hop(pieces[1], "tp", 1)
        return pieces[0].astype(F32) + near.astype(F32) + far.astype(F32)

    def exchange_tp(pieces):
        return [pieces[0]] + [hop(pieces[j], "tp", j) for j in (1, 2, 3)]

    def per_device(layer_input, cotangent, picture_ids, ln1_gain, ln1_bias, w_query, w_key,
                   w_value, query_gain, key_gain, w_out, ln2_gain, ln2_bias, w_hidden,
                   hidden_bias, w_back, out_bias):
        width = layer_input.shape[2]
        piece = layer_input.shape[1]
        heads = w_query.shape[1] // HD
        cells = ctx
        rows = cells * piece
        z = lax.axis_index("ctx")
        t = lax.axis_index("tp")
        y = lax.axis_index("fsdp")

        def to_rows(value):
            parts = [pick(value, z)]
            for by in range(1, ctx):
                parts.append(shift(pick(value, lax.rem(z + by, ctx)), by))
            return jnp.stack(parts)

        def from_rows(value):
            parts = [value[0]] + [shift(value[by], ctx - by) for by in range(1, ctx)]
            stacked = jnp.stack(parts)
            return lax.dynamic_slice_in_dim(
                jnp.concatenate([stacked, stacked]), lax.rem(ctx - z, ctx), ctx, 0)

        def join(value, axis):
            if fsdp != 2:
                return lax.all_gather(value, "fsdp", axis=axis, tiled=True)
            other = hop(value, "fsdp", 1)
            low = jnp.where(y == 0, value, other)
            high = jnp.where(y == 0, other, value)
            return jnp.concatenate([low, high], axis=axis)

        def reduce_grad(value):
            if fsdp == 2:
                half = value.shape[0] // 2
                own = lax.dynamic_slice_in_dim(value, y * half, half, 0)
                sent = lax.dynamic_slice_in_dim(value, (1 - y) * half, half, 0)
                own = add_low(own, hop(sent, "fsdp", 1))
            else:
                own = lax.psum_scatter(value, "fsdp", scatter_dimension=0, tiled=True)
            quarter = own.shape[0] // ctx
            blocks = own.reshape(ctx, quarter, own.shape[1])
            total = pick(blocks, z).astype(F32)
            for by in range(1, ctx):
                total = total + shift(pick(blocks, lax.rem(z + by, ctx)), by).astype(F32)
            return total

        w_qkv = join(jnp.concatenate([w_query, w_key, w_value], axis=1), 0)
        w_pad = jnp.pad(w_qkv.reshape(width, 3 * heads, HD), ((0, 0), (0, 0), (0, LANES - HD)))
        w_pad = w_pad.reshape(width, 3 * heads * LANES)
        lanes = lambda gain: jnp.pad(gain, (0, LANES - HD))[None]
        qg, kg = lanes(query_gain), lanes(key_gain)
        row = lambda vec: vec[None]

        x_own = to_rows(layer_input).reshape(rows, width)
        ids_row = to_rows(picture_ids)
        order = [t, t ^ 1, t ^ 2, t ^ 3]
        ids = [lax.dynamic_slice_in_dim(ids_row, item * piece, piece, 1) for item in order]
        low_id = [jnp.min(jnp.where(item < 0, 1 << 20, item), axis=1) for item in ids]
        high_id = [jnp.max(item, axis=1) for item in ids]
        low_id = jnp.concatenate([jnp.minimum(low_id[0], low_id[1]),
                                  jnp.minimum(low_id[2], low_id[3])])
        high_id = jnp.concatenate([jnp.maximum(high_id[0], high_id[1]),
                                   jnp.maximum(high_id[2], high_id[3])])
        active = ((low_id[:, None] <= high_id[None, :]) & (low_id[None, :] <= high_id[:, None]))
        active = active.astype(jnp.int32)

        x_all = gather_tp(x_own)
        projected = [project(x_all[j], w_pad, row(ln1_gain), row(ln1_bias), qg, kg,
                             ids[j].reshape(rows, 1), heads) for j in range(4)]
        normed = [item[0] for item in projected]
        q = [item[1] for item in projected]
        k = [item[2] for item in projected]
        v = [item[3] for item in projected]

        dy_even = to_rows(lax.dynamic_slice_in_dim(cotangent, t * piece, piece, 1))
        dy_odd = to_rows(lax.dynamic_slice_in_dim(cotangent, (t ^ 2) * piece, piece, 1))
        dy_even, dy_odd = dy_even.reshape(rows, width), dy_odd.reshape(rows, width)
        dy = [dy_even, hop(dy_even, "tp", 1), dy_odd, hop(dy_odd, "tp", 1)]

        w_out_all = gather_tp(join(w_out, 1))
        w_out_full = jnp.concatenate(w_out_all, axis=0)
        full_hidden = join(w_hidden, 0)
        full_back = join(w_back, 1)

        ob2, ob3, of2, of3 = attend(active, q, k, v, 1, heads, cells)
        ob0, ob1, of0, of1 = attend(active, q, k, v, 0, heads, cells)
        ob_full = jnp.concatenate(exchange_tp([ob0, ob1, ob2, ob3]), axis=1)

        attn = dot(ob_full, w_out_full, NN)
        h1 = x_own.astype(F32) + attn
        normal2, scale2 = full_norm(h1)
        mid_own = (normal2 * ln2_gain + ln2_bias).astype(BF16)
        mid = gather_tp(mid_own)
        fed = [feed(mid[j], dy[j], full_hidden, full_back, row(hidden_bias)) for j in range(4)]
        grad_mid = scatter_tp([item[3] for item in fed])
        unit_out = scatter_tp([item[2] for item in fed])
        grad_hidden_bias = jnp.sum(sum(item[4] for item in fed), axis=0)

        layer_output = (h1 + unit_out + out_bias).astype(BF16)
        layer_output = from_rows(layer_output.reshape(cells, piece, width))

        cat = lambda items: jnp.concatenate(items, axis=0)
        mid_cat, du_cat = cat(mid), cat([item[1] for item in fed])
        act_cat, dy_cat = cat([item[0] for item in fed]), cat(dy)
        rows_hidden = reduce_grad(dot(mid_cat, du_cat, TN).astype(BF16))
        rows_back = reduce_grad(dot(dy_cat, act_cat, TN).astype(BF16)).T

        dy_own = dy_even.astype(F32)
        grad_out_bias = jnp.sum(dy_own, axis=0)
        grad_ln2_gain = jnp.sum(grad_mid * normal2, axis=0)
        grad_ln2_bias = jnp.sum(grad_mid, axis=0)
        f2 = grad_mid * ln2_gain
        dh1 = dy_own + scale2 * (
            f2 - jnp.mean(f2, axis=-1, keepdims=True)
            - normal2 * jnp.mean(f2 * normal2, axis=-1, keepdims=True))
        dh1_low = dh1.astype(BF16)
        do_full = [dot(dh1_low, w_out_all[j], NT).astype(BF16) for j in range(4)]
        do = exchange_tp(do_full)
        dq, dk, dv = attend_back(active, q, k, v, do, [of0, of1, of2, of3], heads, cells)
        grad_out = dot(dh1_low, ob_full, TN).astype(BF16)
        feat = heads * HD
        grad_out = scatter_tp([grad_out[:, j * feat:(j + 1) * feat] for j in range(4)])
        rows_out = reduce_grad(grad_out.astype(BF16)).T

        back = [None] * 4
        for j in (3, 2, 1, 0):
            back[j] = project_back(normed[j], w_pad, qg, kg, dq[j], dk[j], dv[j], heads)
        grad_normed = scatter_tp([item[1] for item in back])
        grad_qkv = dot(cat(normed), cat([item[0] for item in back]), TN).astype(BF16)
        rows_qkv = reduce_grad(grad_qkv)

        normal1, scale1 = full_norm(x_own.astype(F32))
        f1 = grad_normed * ln1_gain
        grad_first = scale1 * (
            f1 - jnp.mean(f1, axis=-1, keepdims=True)
            - normal1 * jnp.mean(f1 * normal1, axis=-1, keepdims=True))
        input_grad = from_rows((dh1 + grad_first).astype(BF16).reshape(cells, piece, width))

        vector = jnp.concatenate([
            jnp.sum(grad_normed * normal1, axis=0), jnp.sum(grad_normed, axis=0),
            grad_ln2_gain, grad_ln2_bias, grad_out_bias,
            jnp.sum(sum(item[2] for item in back), axis=0)[:HD],
            jnp.sum(sum(item[3] for item in back), axis=0)[:HD]])

        def butterfly(value, axis):
            bit = 1
            while bit < mesh.shape[axis]:
                value = value + hop(value, axis, bit)
                bit *= 2
            return value

        vector = butterfly(vector, "tp")
        vector = jnp.concatenate([vector, grad_hidden_bias])
        vector = butterfly(butterfly(vector, "fsdp"), "ctx")
        cut = lambda i: vector[i * width:(i + 1) * width]
        tail = 5 * width
        return (
            layer_output, input_grad, cut(0), cut(1),
            rows_qkv[:, :feat], rows_qkv[:, feat:2 * feat], rows_qkv[:, 2 * feat:],
            vector[tail:tail + HD], vector[tail + HD:tail + 2 * HD],
            rows_out, cut(2), cut(3), rows_hidden, vector[tail + 2 * HD:], rows_back, cut(4),
        )

    return jax.shard_map(
        per_device,
        mesh=mesh,
        in_specs=(
            P("fsdp", ("ctx", "tp"), None), P("fsdp", "ctx", None), P("fsdp", "ctx"),
            P(), P(), P("fsdp", "tp"), P("fsdp", "tp"), P("fsdp", "tp"), P(), P(),
            P("tp", "fsdp"), P(), P(), P("fsdp", "tp"), P("tp"), P("tp", "fsdp"), P(),
        ),
        out_specs=(
            P("fsdp", ("ctx", "tp"), None), P("fsdp", ("ctx", "tp"), None), P(), P(),
            P(("fsdp", "ctx"), "tp"), P(("fsdp", "ctx"), "tp"), P(("fsdp", "ctx"), "tp"),
            P(), P(), P("tp", ("fsdp", "ctx")), P(), P(), P(("fsdp", "ctx"), "tp"), P("tp"),
            P("tp", ("fsdp", "ctx")), P(),
        ),
        check_vma=False,
    )
```
